32 devices in a mesh: dp: 1 (over z), pool: 4 (over y), ep: 8 (over x, core).
Axes of the slice: x: 4, y: 4, z: 1, core: 2. Of those that a mesh axis runs over, the one named last changes fastest.
The devices are a block of a 4x4x8 slice.
Arguments:
- hidden: bfloat16 [2048, 1536], P(('dp', 'ep'))
- k_cache: bfloat16 [2, 2048, 128, 2, 128], P(None, ('dp', 'ep'))
- v_cache: bfloat16 [2, 2048, 128, 2, 128], P(None, ('dp', 'ep'))
- lengths: int32 [2048], P(('dp', 'ep'))
- expert_ids: int32 [2, 2048, 4], P(None, ('dp', 'ep'))
- w_query: bfloat16 [2, 1536, 1536], replicated
- w_key: bfloat16 [2, 1536, 256], replicated
- w_value: bfloat16 [2, 1536, 256], replicated
- w_out: bfloat16 [2, 1536, 1536], replicated
- w_router: float32 [2, 1536, 16], replicated
- w_gate: bfloat16 [2, 16, 1536, 2688], P(None, 'ep')
- w_up: bfloat16 [2, 16, 1536, 2688], P(None, 'ep')
- w_down: bfloat16 [2, 16, 2688, 1536], P(None, 'ep')
Outputs:
- output: bfloat16 [2048, 1536], P(('dp', 'ep'))
All inputs are finite; a program needn't handle non-finite values.
Results may differ from the reference program's by a relative error of at most 0.0185129.
Values are sent between devices in bfloat16 or wider.
A program may use at most 768 MiB of HBM per device.

```python
import math
import jax
import jax.numpy as jnp
from jax import lax

LAYERS = 2
D = 1536
FF = 2688
EXPERTS = 16
TOPK = 4
HEADS = 12
KV_HEADS = 2
HEAD = 128
TOK = 128
SEQ = 128
NATT = 16
CAP = 96

EPSILON = 1e-6
ROPE_BASE = 10000.0


def draw_routing(key):
    total = TOK * TOPK
    layers_ids = []
    for layer in range(LAYERS):
        key_hot, key_dev = jax.random.split(jax.random.fold_in(key, layer))
        order = jax.random.permutation(key_hot, EXPERTS)
        n_hot = layer + 1
        n_cold = EXPERTS - n_hot
        spare = total - n_hot * CAP
        base_count = spare // n_cold
        extra_count = spare % n_cold

        def one_block(block_key):
            key_rank, key_tok = jax.random.split(block_key)
            ranks = jax.random.permutation(key_rank, n_cold)
            cold_counts = base_count + (ranks < extra_count).astype(jnp.int32)
            counts = jnp.zeros((EXPERTS,), jnp.int32).at[order[:n_hot]].set(CAP).at[order[n_hot:]].set(cold_counts)
            bounds = jnp.cumsum(counts)
            flat = jnp.sum((bounds[None, :] <= jnp.arange(total)[:, None]).astype(jnp.int32), axis=1)
            table = flat.reshape(TOPK, TOK).T
            return table[jax.random.permutation(key_tok, TOK)]

        block_ids = jax.vmap(one_block)(jax.random.split(key_dev, NATT))
        layers_ids.append(block_ids.reshape(NATT * TOK, TOPK))
    return jnp.stack(layers_ids)


def draw_lengths(key):
    tok_total = NATT * TOK
    key_exp, key_len, key_full = jax.random.split(key, 3)
    top_exp = int(math.log2(SEQ))
    exponent = jax.random.randint(key_exp, (tok_total,), 0, top_exp + 1)
    span = jnp.left_shift(jnp.ones((tok_total,), jnp.int32), exponent)
    lens = 1 + jax.random.randint(key_len, (tok_total,), 0, span)
    return lens.at[jax.random.randint(key_full, (), 0, tok_total)].set(SEQ)


def setup_inputs(seed: int = 0, part: int = 0) -> dict:
    tok_total = NATT * TOK
    base_key = jax.random.key(seed)
    part_key = jax.random.fold_in(jax.random.key(seed + 1), part)
    key_hid, key_kc, key_vc, key_len, key_ids = jax.random.split(part_key, 5)
    keys_w = jax.random.split(base_key, 8)

    def gauss(key, shape, scale):
        return jax.random.normal(key, shape, jnp.float32) * scale

    return {
        "hidden": gauss(key_hid, (tok_total, D), 1.0).astype(jnp.bfloat16),
        "k_cache": gauss(key_kc, (LAYERS, tok_total, SEQ, KV_HEADS, HEAD), 1.0).astype(jnp.bfloat16),
        "v_cache": gauss(key_vc, (LAYERS, tok_total, SEQ, KV_HEADS, HEAD), 1.0).astype(jnp.bfloat16),
        "lengths": draw_lengths(key_len),
        "expert_ids": draw_routing(key_ids),
        "w_query": gauss(keys_w[0], (LAYERS, D, HEADS * HEAD), 1.5 * D ** -0.5).astype(jnp.bfloat16),
        "w_key": gauss(keys_w[1], (LAYERS, D, KV_HEADS * HEAD), D ** -0.5).astype(jnp.bfloat16),
        "w_value": gauss(keys_w[2], (LAYERS, D, KV_HEADS * HEAD), D ** -0.5).astype(jnp.bfloat16),
        "w_out": gauss(keys_w[3], (LAYERS, HEADS * HEAD, D), 2.0 * (HEADS * HEAD) ** -0.5).astype(jnp.bfloat16),
        "w_router": gauss(keys_w[4], (LAYERS, D, EXPERTS), 1.5 * D ** -0.5),
        "w_gate": gauss(keys_w[5], (LAYERS, EXPERTS, D, FF), D ** -0.5).astype(jnp.bfloat16),
        "w_up": gauss(keys_w[6], (LAYERS, EXPERTS, D, FF), D ** -0.5).astype(jnp.bfloat16),
        "w_down": gauss(keys_w[7], (LAYERS, EXPERTS, FF, D), 2.0 * FF ** -0.5).astype(jnp.bfloat16),
    }


def rms_normed(values):
    return values * lax.rsqrt(jnp.mean(values * values, axis=-1, keepdims=True) + EPSILON)


def rotary(vectors, positions):
    half = vectors.shape[-1] // 2
    freqs = ROPE_BASE ** (-2.0 * jnp.arange(half, dtype=jnp.float32) / vectors.shape[-1])
    angle = positions[:, None, None] * freqs[None, None, :]
    cosine = jnp.cos(angle)
    sine = jnp.sin(angle)
    first = vectors[..., :half]
    second = vectors[..., half:]
    return jnp.concatenate([first * cosine - second * sine, second * cosine + first * sine], axis=-1)


def attend_block(hidden_blk, keys_blk, vals_blk, lens_blk, w_q, w_k, w_v, w_o):
    hidden_f = hidden_blk.astype(jnp.float32)
    normed = rms_normed(hidden_f).astype(jnp.bfloat16)
    positions = lens_blk.astype(jnp.float32)
    query = rotary(jnp.dot(normed, w_q, preferred_element_type=jnp.float32).reshape(TOK, HEADS, HEAD), positions)
    query = query.astype(jnp.bfloat16).reshape(TOK, KV_HEADS, HEADS // KV_HEADS, HEAD).astype(jnp.float32)
    key_new = rotary(jnp.dot(normed, w_k, preferred_element_type=jnp.float32).reshape(TOK, KV_HEADS, HEAD), positions)
    key_new = key_new.astype(jnp.bfloat16).astype(jnp.float32)
    val_new = jnp.dot(normed, w_v, preferred_element_type=jnp.float32).astype(jnp.bfloat16).reshape(TOK, KV_HEADS, HEAD)
    scale = HEAD ** -0.5
    scores = jnp.einsum("tkgd,tskd->tkgs", query, keys_blk.astype(jnp.float32)) * scale
    valid = jnp.arange(SEQ)[None, None, None, :] < lens_blk[:, None, None, None]
    scores = jnp.where(valid, scores, -jnp.inf)
    score_new = jnp.einsum("tkgd,tkd->tkg", query, key_new) * scale
    peak = jnp.maximum(jnp.max(scores, axis=-1), score_new)
    weights = jnp.exp(scores - peak[..., None])
    weight_new = jnp.exp(score_new - peak)
    denominator = jnp.sum(weights, axis=-1) + weight_new
    mixed = jnp.einsum("tkgs,tskd->tkgd", weights.astype(jnp.bfloat16).astype(jnp.float32), vals_blk.astype(jnp.float32))
    mixed = mixed + weight_new.astype(jnp.bfloat16).astype(jnp.float32)[..., None] * val_new.astype(jnp.float32)[:, :, None, :]
    attended = (mixed / denominator[..., None]).astype(jnp.bfloat16).reshape(TOK, HEADS * HEAD)
    return (hidden_f + jnp.dot(attended, w_o, preferred_element_type=jnp.float32)).astype(jnp.bfloat16)


def moe_layer(attn_out, ids_layer, w_r, w_gate, w_up, w_down):
    residual = attn_out.astype(jnp.float32)
    mixed_in = rms_normed(residual).astype(jnp.bfloat16)
    logits = jnp.dot(mixed_in.astype(jnp.float32), w_r)
    gates = jax.nn.softmax(jnp.take_along_axis(logits, ids_layer, axis=1), axis=-1)
    blocks_in = mixed_in.reshape(NATT, TOK, D).astype(jnp.float32)
    id_blocks = ids_layer.reshape(NATT, TOK, TOPK)
    gate_blocks = gates.reshape(NATT, TOK, TOPK)
    slot_ids = jnp.arange(CAP)

    def step(total_acc, layer_pack):
        expert, w_one, w_three, w_two = layer_pack
        hit = id_blocks == expert
        weight = jnp.sum(jnp.where(hit, gate_blocks, 0.0), axis=2)
        chosen = jnp.any(hit, axis=2)
        rank = jnp.cumsum(chosen.astype(jnp.int32), axis=1) - 1
        select = ((rank[:, None, :] == slot_ids[None, :, None]) & chosen[:, None, :]).astype(jnp.float32)
        rows = jnp.einsum("bct,btd->bcd", select, blocks_in).astype(jnp.bfloat16).reshape(NATT * CAP, D)
        inner = jax.nn.silu(jnp.dot(rows, w_one, preferred_element_type=jnp.float32)) * jnp.dot(rows, w_three, preferred_element_type=jnp.float32)
        result = jnp.dot(inner.astype(jnp.bfloat16), w_two, preferred_element_type=jnp.float32).astype(jnp.bfloat16)
        back = jnp.einsum("bct,bcd->btd", select, result.reshape(NATT, CAP, D).astype(jnp.float32))
        return total_acc + weight[:, :, None] * back, None

    total_acc, _ = lax.scan(step, jnp.zeros((NATT, TOK, D), jnp.float32), (jnp.arange(EXPERTS), w_gate, w_up, w_down))
    return (residual + total_acc.reshape(NATT * TOK, D)).astype(jnp.bfloat16)


def reference(hidden, k_cache, v_cache, lengths, expert_ids, w_query, w_key, w_value, w_out, w_router, w_gate, w_up, w_down):
    def layer_step(state, layer_pack):
        cache_k, cache_v, ids_layer, w_q, w_k, w_v, w_o, w_r, w_one, w_three, w_two = layer_pack

        def per_block(block_in):
            return attend_block(block_in[0], block_in[1], block_in[2], block_in[3], w_q, w_k, w_v, w_o)

        attn_out = lax.map(per_block, (state.reshape(NATT, TOK, D), cache_k.reshape(NATT, TOK, SEQ, KV_HEADS, HEAD), cache_v.reshape(NATT, TOK, SEQ, KV_HEADS, HEAD), lengths.reshape(NATT, TOK)))
        return moe_layer(attn_out.reshape(NATT * TOK, D), ids_layer, w_r, w_one, w_three, w_two), None

    final, _ = lax.scan(layer_step, hidden, (k_cache, v_cache, expert_ids, w_query, w_key, w_value, w_out, w_router, w_gate, w_up, w_down))
    return final
```

```python
import functools

import jax
import jax.numpy as jnp
from jax import lax
from jax.experimental import pallas as pl
from jax.experimental.pallas import tpu as pltpu
from jax.sharding import PartitionSpec as P

EPSILON = 1e-6
ROPE_BASE = 10000.0
MESH = pl.DeviceIdType.MESH
F32 = jnp.float32
BF16 = jnp.bfloat16
CORES = 2
HP = 16
LANES = 128
NW = 384
NS = 512
R13 = 3


def step_kernel(cfg, x_hbm, kc_hbm, vc_hbm, len_ref, ids_ref, wq_hbm, wk_hbm, wv_hbm, wo_hbm, wr_ref, wg_hbm, wu_hbm, wd_hbm,
                out_hbm,
                xin, xs, a_scr, q_scr, kn_scr, vn_scr, mn_scr, den_scr, s_scr, p_scr, cos_scr, sin_scr, wr3,
                kbuf, vbuf, wqb, wkb, wvb, wob, w13, w2b,
                u_all, g_all, gcol, inner, psum, pairbuf, rbuf, fin,
                sem_x, sem_w, sem_k, sem_v, sem_g, sem_u, sem_d,
                du_s, du_r, dg_s, dg_r, pr_s, pr_r, rr_s, rr_r, fs, fr, sem_o):
    layers, tok, model, heads, kvh, hd, seq, ff, nloc, nx, npool, nexp, topk = cfg
    ep = nx * CORES
    rows = ep * tok
    half = tok // 2
    group = heads // kvh
    pool = lax.axis_index("pool")
    e = lax.axis_index("ep")
    xx = lax.div(e, CORES)
    c = lax.rem(e, CORES)
    oc = 1 - c
    xr = lax.rem(xx + 1, nx)
    xl = lax.rem(xx + nx - 1, nx)
    xf = lax.rem(xx + 2, nx)
    partner = xx * CORES + oc
    er = xr * CORES + c
    el = xl * CORES + c
    ef = xf * CORES + c
    pn = lax.rem(pool + 1, npool)
    pp = lax.rem(pool + npool - 1, npool)
    pf = lax.rem(pool + 2, npool)

    def to_ep(i):
        return {"ep": i}

    def to_pool(i):
        return {"pool": i}

    barrier = pltpu.get_barrier_semaphore()
    for dev in (to_ep(partner), to_ep(er), to_ep(el), to_pool(pn), to_pool(pp)):
        pl.semaphore_signal(barrier, inc=1, device_id=dev, device_id_type=MESH)

    kpieces = sem_k.shape[0]
    kp = tok // kpieces
    tok0 = pl.multiple_of(pool * tok, tok)

    def k_copy(l, i):
        return pltpu.make_async_copy(kc_hbm.at[l, pl.ds(tok0 + i * kp, kp)], kbuf.at[pl.ds(i * kp, kp)], sem_k.at[i])

    def v_copy(l, i):
        return pltpu.make_async_copy(vc_hbm.at[l, pl.ds(tok0 + i * kp, kp)], vbuf.at[pl.ds(i * kp, kp)], sem_v.at[i])

    def w_copy(l, i):
        src = (wq_hbm, wk_hbm, wv_hbm, wo_hbm)[i]
        dst = (wqb, wkb, wvb, wob)[i]
        return pltpu.make_async_copy(src.at[l], dst, sem_w.at[i])

    n13 = ff // NW
    n2 = model // NS
    tot13 = layers * nloc * n13
    tot2 = layers * nloc * n2

    def g_copies(t):
        li = lax.div(t, n13)
        j = lax.rem(t, n13)
        l = lax.div(li, nloc)
        i = lax.rem(li, nloc)
        slot = lax.rem(t, R13)
        cols = pl.ds(pl.multiple_of(j * NW, NW), NW)
        return (pltpu.make_async_copy(wg_hbm.at[l, i, :, cols], w13.at[slot, :, pl.ds(0, NW)], sem_g.at[slot]),
                pltpu.make_async_copy(wu_hbm.at[l, i, :, cols], w13.at[slot, :, pl.ds(NW, NW)], sem_u.at[slot]))

    def d_copy(t):
        li = lax.div(t, n2)
        j = lax.rem(t, n2)
        l = lax.div(li, nloc)
        i = lax.rem(li, nloc)
        cols = pl.ds(pl.multiple_of(j * NS, NS), NS)
        return pltpu.make_async_copy(wd_hbm.at[l, i, :, cols], w2b.at[j], sem_d.at[j])

    x_copy = pltpu.make_async_copy(x_hbm.at[pl.ds(tok0, tok)], xin, sem_x.at[0])
    x_copy.start()
    for i in range(3):
        w_copy(0, i).start()
    for i in range(kpieces):
        k_copy(0, i).start()

    lane = lax.broadcasted_iota(jnp.int32, (tok, hd), 1)
    pos_i = jnp.zeros((tok, hd), jnp.int32)
    row_i = lax.broadcasted_iota(jnp.int32, (tok, hd), 0)
    for t in range(tok):
        pos_i = jnp.where(row_i == t, len_ref[pool * tok + t], pos_i)
    half_hd = hd // 2
    pair = jnp.where(lane < half_hd, lane, lane - half_hd).astype(F32)
    freqs = jnp.exp(pair * (-2.0 / hd) * jnp.log(jnp.full((tok, hd), ROPE_BASE, F32)))
    angle = pos_i.astype(F32) * freqs
    cos_scr[...] = jnp.cos(angle)
    sn = jnp.sin(angle)
    sin_scr[...] = jnp.where(lane < half_hd, -sn, sn)
    for l in range(layers):
        w = wr_ref[l]
        hi = w.astype(BF16)
        r1 = w - hi.astype(F32)
        mid = r1.astype(BF16)
        lo = (r1 - mid.astype(F32)).astype(BF16)
        wr3[l, pl.ds(0, nexp), :] = hi
        wr3[l, pl.ds(nexp, nexp), :] = mid
        wr3[l, pl.ds(2 * nexp, nexp), :] = lo
    zero_rows = jnp.zeros((tok, hd), F32)
    for h in range(heads, HP):
        q_scr[pl.ds(h, tok, stride=HP), :] = zero_rows
        kn_scr[pl.ds(h, tok, stride=HP), :] = zero_rows
        vn_scr[pl.ds(h, tok, stride=HP), :] = zero_rows

    pl.semaphore_wait(barrier, 5)
    x_copy.wait()
    xs[...] = xin[...].astype(F32)

    scale = hd ** -0.5
    rix = lax.broadcasted_iota(jnp.int32, (HP, seq * kvh), 0)
    cix = lax.broadcasted_iota(jnp.int32, (HP, seq * kvh), 1)
    own_kv = lax.rem(cix, kvh) == lax.div(rix, group)
    colpos = jnp.where(own_kv, lax.div(cix, kvh), 2 * seq)

    def rotate(v):
        return v * cos_scr[...] + pltpu.roll(v, half_hd, 1) * sin_scr[...]

    def attention(l):
        xf32 = xs[...]
        h = (xf32 * lax.rsqrt(jnp.mean(xf32 * xf32, axis=-1, keepdims=True) + EPSILON)).astype(BF16)
        w_copy(l, 0).wait()
        per = 256 // hd
        for n in range(heads // per):
            qn = jnp.dot(h, wqb[:, n * 256:(n + 1) * 256], preferred_element_type=F32)
            for s in range(per):
                r = rotate(qn[:, s * hd:(s + 1) * hd]).astype(BF16).astype(F32)
                q_scr[pl.ds(n * per + s, tok, stride=HP), :] = r
        w_copy(l, 1).wait()
        kn = jnp.dot(h, wkb[...], preferred_element_type=F32)
        w_copy(l, 2).wait()
        vn = jnp.dot(h, wvb[...], preferred_element_type=F32)
        for kv in range(kvh):
            r = rotate(kn[:, kv * hd:(kv + 1) * hd]).astype(BF16).astype(F32)
            v = vn[:, kv * hd:(kv + 1) * hd].astype(BF16).astype(F32)
            for g in range(group):
                kn_scr[pl.ds(kv * group + g, tok, stride=HP), :] = r
                vn_scr[pl.ds(kv * group + g, tok, stride=HP), :] = v
        if l == 0:
            for i in range(kpieces):
                v_copy(l, i).start()
            w_copy(l, 3).start()

        def qk(i, carry):
            k_copy(l, i).wait()
            for s in range(kp):
                t = i * kp + s
                r16 = pl.ds(pl.multiple_of(t * HP, HP), HP)
                q = q_scr[r16, :].astype(BF16)
                sc = lax.dot_general(q, kbuf[t], (((1,), (1,)), ((), ())), preferred_element_type=F32)
                s_scr[r16, :] = jnp.where(colpos < len_ref[pool * tok + t], sc * scale, -jnp.inf)
            return carry

        lax.fori_loop(0, kpieces, qk, 0)
        if l == 0:
            for t in range(R13):
                for cp in g_copies(t):
                    cp.start()

        def soft(i, carry):
            rr = pl.ds(pl.multiple_of(i * 128, 128), 128)
            sc = s_scr[rr, :]
            s_new = jnp.sum(q_scr[rr, :] * kn_scr[rr, :], axis=-1, keepdims=True) * scale
            peak = jnp.maximum(jnp.max(sc, axis=-1, keepdims=True), s_new)
            wts = jnp.exp(sc - peak)
            w_new = jnp.exp(s_new - peak)
            den = jnp.sum(wts, axis=-1, keepdims=True) + w_new
            p_scr[rr, :] = wts.astype(BF16)
            mn_scr[rr, :] = w_new.astype(BF16).astype(F32) * vn_scr[rr, :]
            den_scr[rr, :] = jnp.broadcast_to(den, (128, hd))
            return carry

        lax.fori_loop(0, tok * HP // 128, soft, 0)

        def pv(i, carry):
            v_copy(l, i).wait()
            for s in range(kp):
                t = i * kp + s
                r16 = pl.ds(pl.multiple_of(t * HP, HP), HP)
                m = jnp.dot(p_scr[r16, :], vbuf[t], preferred_element_type=F32)
                mn_scr[r16, :] = ((m + mn_scr[r16, :]) / den_scr[r16, :]).astype(BF16).astype(F32)
            return carry

        lax.fori_loop(0, kpieces, pv, 0)
        att = jnp.concatenate([mn_scr[pl.ds(h, tok, stride=HP), :].astype(BF16) for h in range(heads)], axis=1)
        w_copy(l, 3).wait()
        for n in range(model // 256):
            cs = slice(n * 256, (n + 1) * 256)
            a_scr[:, cs] = (xs[:, cs] + jnp.dot(att, wob[:, cs], preferred_element_type=F32)).astype(BF16).astype(F32)
        a = a_scr[...]
        u = (a * lax.rsqrt(jnp.mean(a * a, axis=-1, keepdims=True) + EPSILON)).astype(BF16)
        u_all[pl.ds(pl.multiple_of(e * tok, tok), tok), :] = u
        parts = lax.dot_general(wr3[l], u, (((1,), (1,)), ((), ())), preferred_element_type=F32)
        logits = (parts[2 * nexp:3 * nexp] + parts[nexp:2 * nexp]) + parts[0:nexp]
        ids = ids_ref[l]
        mine = ids[:, 0:tok]
        for i in range(1, npool):
            mine = jnp.where(pool == i, ids[:, i * tok:(i + 1) * tok], mine)
        eix = lax.broadcasted_iota(jnp.int32, (nexp, tok), 0)
        hit = eix == mine[0:1, :]
        for k in range(1, topk):
            hit = jnp.logical_or(hit, eix == mine[k:k + 1, :])
        ml = jnp.where(hit, logits, -jnp.inf)
        ex = jnp.exp(ml - jnp.max(ml, axis=0, keepdims=True))
        gates = ex / jnp.sum(ex, axis=0, keepdims=True)
        g_all[e] = jnp.concatenate([gates, jnp.zeros((nexp, LANES - tok), F32)], axis=1)

    def blk(i):
        return pl.ds(pl.multiple_of(i * tok, tok), tok)

    def hblk(i, s):
        return pl.ds(pl.multiple_of(i * tok + s * half, half), half)

    def dcopy(i, dev, rws, gix):
        a = pltpu.make_async_remote_copy(src_ref=u_all.at[rws], dst_ref=u_all.at[rws], send_sem=du_s.at[i], recv_sem=du_r.at[i],
                                         device_id=dev, device_id_type=MESH)
        if gix is None:
            return (a,)
        b = pltpu.make_async_remote_copy(src_ref=g_all.at[gix], dst_ref=g_all.at[gix], send_sem=dg_s.at[i], recv_sem=dg_r.at[i],
                                         device_id=dev, device_id_type=MESH)
        return (a, b)

    def start(cs):
        for cp in cs:
            cp.start()

    def wait_recv(cs):
        for cp in cs:
            cp.wait_recv()

    def wait_send(cs):
        for cp in cs:
            cp.wait_send()

    def dispatch():
        t1 = dcopy(1, to_ep(er), blk(e), e)
        t2 = dcopy(2, to_ep(el), blk(e), e)
        t0 = dcopy(0, to_ep(partner), blk(e), e)
        start(t1)
        start(t2)
        start(t0)
        wait_recv(t1)
        t3 = dcopy(3, to_ep(er), hblk(el, 0), el)
        start(t3)
        t5 = dcopy(5, to_ep(partner), blk(el), el)
        start(t5)
        wait_recv(t2)
        t4 = dcopy(4, to_ep(el), hblk(er, 1), None)
        start(t4)
        t6 = dcopy(6, to_ep(partner), blk(er), er)
        start(t6)
        wait_recv(t3)
        wait_recv(t4)
        t7 = dcopy(7, to_ep(partner), blk(ef), ef)
        start(t7)
        for t in (t0, t5, t6, t7):
            wait_recv(t)
        return (t0, t1, t2, t3, t4, t5, t6, t7)

    def gate_columns():
        gt = jnp.transpose(g_all[...].reshape(ep * nexp, LANES))
        gt = gt[0:tok, :]
        lix = lax.broadcasted_iota(jnp.int32, (tok, ep * nexp), 1)
        for i in range(nloc):
            for b in range(ep):
                col = jnp.sum(jnp.where(lix == b * nexp + e * nloc + i, gt, 0.0), axis=1, keepdims=True)
                gcol[i, pl.ds(b * tok, tok), :] = jnp.broadcast_to(col, (tok, LANES))

    def experts(l, i):
        base13 = (l * nloc + i) * n13
        base2 = (l * nloc + i) * n2

        def up(j, carry):
            t = base13 + j
            slot = lax.rem(t, R13)
            for cp in g_copies(t):
                cp.wait()
            hh = jnp.dot(u_all[...], w13[slot], preferred_element_type=F32)
            gate = hh[:, 0:NW]
            act = gate * jax.nn.sigmoid(gate) * hh[:, NW:2 * NW]
            inner[:, pl.ds(pl.multiple_of(j * NW, NW), NW)] = act.astype(BF16)

            @pl.when(t + R13 < tot13)
            def _():
                for cp in g_copies(t + R13):
                    cp.start()
            return carry

        lax.fori_loop(0, n13, up, 0)

        def down(j, carry):
            t = base2 + j
            d_copy(t).wait()
            y = jnp.dot(inner[...], w2b[j], preferred_element_type=F32).astype(BF16).astype(F32)
            gc = gcol[i]
            for s in range(NS // LANES):
                ys = y[:, s * LANES:(s + 1) * LANES]
                term = jnp.where(gc > 0.0, gc * ys, 0.0)
                cols = pl.ds(pl.multiple_of(j * NS + s * LANES, LANES), LANES)
                if i == 0:
                    psum[:, cols] = term
                else:
                    psum[:, cols] = psum[:, cols] + term

            @pl.when(t + n2 < tot2)
            def _():
                d_copy(t + n2).start()
            return carry

        lax.fori_loop(0, n2, down, 0)

    def rcopy(i, dev, rws):
        return pltpu.make_async_remote_copy(src_ref=psum.at[rws], dst_ref=rbuf.at[i], send_sem=rr_s.at[i], recv_sem=rr_r.at[i],
                                            device_id=dev, device_id_type=MESH)

    def give_back():
        order = (xf, xr, xl, xx)
        pairs = []
        for k in range(nx):
            cp = pltpu.make_async_remote_copy(src_ref=psum.at[blk(order[k] * CORES + oc)], dst_ref=pairbuf.at[k], send_sem=pr_s.at[k],
                                              recv_sem=pr_r.at[k], device_id=to_ep(partner), device_id_type=MESH)
            cp.start()
            pairs.append(cp)

        def add_pair(k):
            pairs[k].wait_recv()
            rws = blk(order[k] * CORES + c)
            psum[rws, :] = psum[rws, :] + pairbuf[k]

        m0 = rcopy(0, to_ep(er), hblk(ef, 1))
        m1 = rcopy(1, to_ep(el), hblk(ef, 0))
        m2 = rcopy(2, to_ep(er), hblk(er, 0))
        m3 = rcopy(3, to_ep(el), hblk(el, 1))
        m4 = rcopy(4, to_ep(er), hblk(er, 1))
        m5 = rcopy(5, to_ep(el), hblk(el, 0))
        add_pair(0)
        m0.start()
        m1.start()
        add_pair(1)
        m2.start()
        add_pair(2)
        m3.start()
        m0.wait_recv()
        psum[hblk(er, 1), :] = psum[hblk(er, 1), :] + rbuf[0]
        m4.start()
        m1.wait_recv()
        psum[hblk(el, 0), :] = psum[hblk(el, 0), :] + rbuf[1]
        m5.start()
        add_pair(3)
        m2.wait_recv()
        psum[hblk(e, 0), :] = psum[hblk(e, 0), :] + rbuf[2]
        m3.wait_recv()
        psum[hblk(e, 1), :] = psum[hblk(e, 1), :] + rbuf[3]
        m5.wait_recv()
        xs[0:half, :] = (a_scr[0:half, :] + (psum[hblk(e, 0), :] + rbuf[5])).astype(BF16).astype(F32)
        m4.wait_recv()
        xs[half:tok, :] = (a_scr[half:tok, :] + (psum[hblk(e, 1), :] + rbuf[4])).astype(BF16).astype(F32)
        wait_send(pairs)
        wait_send((m0, m1, m2, m3, m4, m5))

    for l in range(layers):
        attention(l)
        sent = dispatch()
        gate_columns()
        if l == 0:
            for t in range(n2):
                d_copy(t).start()
        for i in range(nloc):
            experts(l, i)
            if i == 0 and l + 1 < layers:
                for k in range(4):
                    w_copy(l + 1, k).start()
                for k in range(kpieces):
                    k_copy(l + 1, k).start()
                    v_copy(l + 1, k).start()
        for s in sent:
            wait_send(s)
        give_back()

    def fcopy(i, dev, rws):
        return pltpu.make_async_remote_copy(src_ref=fin.at[rws], dst_ref=fin.at[rws], send_sem=fs.at[i], recv_sem=fr.at[i],
                                            device_id=dev, device_id_type=MESH)

    def ocopy(i):
        return pltpu.make_async_copy(fin.at[blk(i)], out_hbm.at[blk(i)], sem_o.at[i])

    fin[blk(pool), :] = xs[...].astype(BF16)
    f0 = fcopy(0, to_pool(pn), blk(pool))
    f1 = fcopy(1, to_pool(pp), blk(pool))
    f0.start()
    f1.start()
    ocopy(pool).start()
    f0.wait_recv()
    f2 = fcopy(2, to_pool(pn), hblk(pp, 0))
    f2.start()
    ocopy(pp).start()
    f1.wait_recv()
    f3 = fcopy(3, to_pool(pp), hblk(pn, 1))
    f3.start()
    ocopy(pn).start()
    f2.wait_recv()
    f3.wait_recv()
    ocopy(pf).start()
    for i in (pool, pp, pn, pf):
        ocopy(i).wait()
    wait_send((f0, f1, f2, f3))


def solution(mesh):
    npool = mesh.shape["pool"]
    ep = mesh.shape["ep"]
    nx = ep // CORES

    def body(hidden, k_cache, v_cache, lengths, expert_ids, w_query, w_key, w_value, w_out, w_router, w_gate, w_up, w_down):
        layers, local, seq, kvh, hd = k_cache.shape
        model = hidden.shape[1]
        tok = local // npool
        heads = w_query.shape[2] // hd
        nloc, _, ff = w_gate.shape[1:]
        nexp = w_router.shape[2]
        topk = expert_ids.shape[2]
        kc = k_cache.reshape(layers, local, seq * kvh, hd)
        vc = v_cache.reshape(layers, local, seq * kvh, hd)
        ids_t = expert_ids.transpose(0, 2, 1)
        wr_t = w_router.transpose(0, 2, 1)
        cfg = (layers, tok, model, heads, kvh, hd, seq, ff, nloc, nx, npool, nexp, topk)
        rows = ep * tok
        half = tok // 2
        hbm = pl.BlockSpec(memory_space=pl.ANY)
        vmem = pl.BlockSpec(memory_space=pltpu.VMEM)
        smem = pl.BlockSpec(memory_space=pltpu.SMEM)
        kpieces = 8
        dma = pltpu.SemaphoreType.DMA
        n2 = model // NS
        scratch = [
            pltpu.VMEM((tok, model), BF16), pltpu.VMEM((tok, model), F32), pltpu.VMEM((tok, model), F32),
            pltpu.VMEM((tok * HP, hd), F32), pltpu.VMEM((tok * HP, hd), F32), pltpu.VMEM((tok * HP, hd), F32),
            pltpu.VMEM((tok * HP, hd), F32), pltpu.VMEM((tok * HP, hd), F32),
            pltpu.VMEM((tok * HP, seq * kvh), F32), pltpu.VMEM((tok * HP, seq * kvh), BF16),
            pltpu.VMEM((tok, hd), F32), pltpu.VMEM((tok, hd), F32), pltpu.VMEM((layers, 3 * nexp, model), BF16),
            pltpu.VMEM((tok, seq * kvh, hd), BF16), pltpu.VMEM((tok, seq * kvh, hd), BF16),
            pltpu.VMEM((model, heads * hd), BF16), pltpu.VMEM((model, kvh * hd), BF16), pltpu.VMEM((model, kvh * hd), BF16),
            pltpu.VMEM((heads * hd, model), BF16),
            pltpu.VMEM((R13, model, 2 * NW), BF16), pltpu.VMEM((n2, ff, NS), BF16),
            pltpu.VMEM((rows, model), BF16), pltpu.VMEM((ep, nexp, LANES), F32), pltpu.VMEM((nloc, rows, LANES), F32),
            pltpu.VMEM((rows, ff), BF16), pltpu.VMEM((rows, model), F32), pltpu.VMEM((nx, tok, model), F32),
            pltpu.VMEM((6, half, model), F32), pltpu.VMEM((local, model), BF16),
            dma((1,)), dma((4,)), dma((kpieces,)), dma((kpieces,)), dma((R13,)), dma((R13,)), dma((n2,)),
            dma((8,)), dma((8,)), dma((8,)), dma((8,)), dma((nx,)), dma((nx,)), dma((6,)), dma((6,)), dma((4,)), dma((4,)),
            dma((npool,)),
        ]
        call = pl.pallas_call(
            functools.partial(step_kernel, cfg),
            out_shape=jax.ShapeDtypeStruct((local, model), BF16),
            in_specs=[hbm, hbm, hbm, smem, vmem, hbm, hbm, hbm, hbm, vmem, hbm, hbm, hbm],
            out_specs=hbm,
            scratch_shapes=scratch,
            compiler_params=pltpu.CompilerParams(collective_id=0, has_side_effects=True, vmem_limit_bytes=66_000_000),
        )
        return call(hidden, kc, vc, lengths, ids_t, w_query, w_key, w_value, w_out, wr_t, w_gate, w_up, w_down)

    rows_spec = ("dp", "ep")
    in_specs = (P(rows_spec, None), P(None, rows_spec), P(None, rows_spec), P(rows_spec), P(None, rows_spec, None), P(), P(), P(), P(), P(), P(None, "ep"), P(None, "ep"), P(None, "ep"))
    return jax.shard_map(body, mesh=mesh, in_specs=in_specs, out_specs=P(rows_spec, None), check_vma=False)
```

```python
import functools

import jax
import jax.numpy as jnp
from jax import lax
from jax.experimental import pallas as pl
from jax.experimental.pallas import tpu as pltpu
from jax.sharding import PartitionSpec as P

EPSILON = 1e-6
ROPE_BASE = 10000.0
MESH = pl.DeviceIdType.MESH
F32 = jnp.float32
BF16 = jnp.bfloat16
CORES = 2
HP = 16
LANES = 128
NW = 384
R13 = 4
HALVES = 2


def step_kernel(cfg, x_hbm, kc_hbm, vc_hbm, len_ref, ids_ref, wq_hbm, wk_hbm, wv_hbm, wo_hbm, wr_ref, wg_hbm, wu_hbm, wd_hbm,
                out_hbm,
                xin, xs, a_scr, q_scr, kn_scr, vn_scr, mn_scr, den_scr, s_scr, p_scr, cos_scr, sin_scr, wr3,
                kbuf, vbuf, wqb, wkb, wvb, wob, w13, w2b,
                u_all, g_all, gcol, inner, psum, pairbuf, rbuf, fin,
                sem_x, sem_w, sem_k, sem_v, sem_g, sem_u, sem_d,
                du_s, du_r, dg_s, dg_r, pr_s, pr_r, rr_s, rr_r, fs, fr, sem_o):
    layers, tok, model, heads, kvh, hd, seq, ff, nloc, nx, npool, nexp, topk = cfg
    ep = nx * CORES
    rows = ep * tok
    ht = tok // HALVES
    hrows = rows // HALVES
    half = ht // 2
    group = heads // kvh
    pool = lax.axis_index("pool")
    e = lax.axis_index("ep")
    xx = lax.div(e, CORES)
    c = lax.rem(e, CORES)
    oc = 1 - c
    xr = lax.rem(xx + 1, nx)
    xl = lax.rem(xx + nx - 1, nx)
    xf = lax.rem(xx + 2, nx)
    partner = xx * CORES + oc
    dr = xr * CORES + oc
    dl = xl * CORES + oc
    er = xr * CORES + c
    el = xl * CORES + c
    ef = xf * CORES + c
    pn = lax.rem(pool + 1, npool)
    pp = lax.rem(pool + npool - 1, npool)
    pf = lax.rem(pool + 2, npool)

    def to_ep(i):
        return {"ep": i}

    def to_pool(i):
        return {"pool": i}

    barrier = pltpu.get_barrier_semaphore()
    for dev in (to_ep(partner), to_ep(er), to_ep(el), to_ep(dr), to_ep(dl), to_pool(pn), to_pool(pp)):
        pl.semaphore_signal(barrier, inc=1, device_id=dev, device_id_type=MESH)

    kpieces = sem_k.shape[0]
    kp = tok // kpieces
    tok0 = pl.multiple_of(pool * tok, tok)

    def k_copy(l, i):
        return pltpu.make_async_copy(kc_hbm.at[l, pl.ds(tok0 + i * kp, kp)], kbuf.at[pl.ds(i * kp, kp)], sem_k.at[i])

    def v_copy(l, i):
        return pltpu.make_async_copy(vc_hbm.at[l, pl.ds(tok0 + i * kp, kp)], vbuf.at[pl.ds(i * kp, kp)], sem_v.at[i])

    def w_copy(l, i):
        src = (wq_hbm, wk_hbm, wv_hbm, wo_hbm)[i]
        dst = (wqb, wkb, wvb, wob)[i]
        return pltpu.make_async_copy(src.at[l], dst, sem_w.at[i])

    n13 = ff // NW
    npass = nloc * HALVES
    tot13 = layers * npass * n13
    tot2 = layers * nloc

    def g_copies(t):
        lq = lax.div(t, n13)
        j = lax.rem(t, n13)
        l = lax.div(lq, npass)
        i = lax.div(lax.rem(lq, npass), HALVES)
        slot = lax.rem(t, R13)
        cols = pl.ds(pl.multiple_of(j * NW, NW), NW)
        return (pltpu.make_async_copy(wg_hbm.at[l, i, :, cols], w13.at[slot, :, pl.ds(0, NW)], sem_g.at[slot]),
                pltpu.make_async_copy(wu_hbm.at[l, i, :, cols], w13.at[slot, :, pl.ds(NW, NW)], sem_u.at[slot]))

    def d_copy(t):
        return pltpu.make_async_copy(wd_hbm.at[t // nloc, t % nloc], w2b, sem_d.at[0])

    x_copy = pltpu.make_async_copy(x_hbm.at[pl.ds(tok0, tok)], xin, sem_x.at[0])
    x_copy.start()
    for i in range(3):
        w_copy(0, i).start()
    for i in range(kpieces):
        k_copy(0, i).start()

    lane = lax.broadcasted_iota(jnp.int32, (tok, hd), 1)
    pos_i = jnp.zeros((tok, hd), jnp.int32)
    row_i = lax.broadcasted_iota(jnp.int32, (tok, hd), 0)
    for t in range(tok):
        pos_i = jnp.where(row_i == t, len_ref[pool * tok + t], pos_i)
    half_hd = hd // 2
    pair = jnp.where(lane < half_hd, lane, lane - half_hd).astype(F32)
    freqs = jnp.exp(pair * (-2.0 / hd) * jnp.log(jnp.full((tok, hd), ROPE_BASE, F32)))
    angle = pos_i.astype(F32) * freqs
    cos_scr[...] = jnp.cos(angle)
    sn = jnp.sin(angle)
    sin_scr[...] = jnp.where(lane < half_hd, -sn, sn)
    for l in range(layers):
        w = wr_ref[l]
        hi = w.astype(BF16)
        r1 = w - hi.astype(F32)
        mid = r1.astype(BF16)
        lo = (r1 - mid.astype(F32)).astype(BF16)
        wr3[l, pl.ds(0, nexp), :] = hi
        wr3[l, pl.ds(nexp, nexp), :] = mid
        wr3[l, pl.ds(2 * nexp, nexp), :] = lo
    zero_rows = jnp.zeros((ht, hd), F32)
    for h in range(heads, HP):
        q_scr[pl.ds(h, ht, stride=HP), :] = zero_rows
        kn_scr[pl.ds(h, ht, stride=HP), :] = zero_rows
        vn_scr[pl.ds(h, ht, stride=HP), :] = zero_rows

    pl.semaphore_wait(barrier, 7)
    x_copy.wait()
    xs[...] = xin[...].astype(F32)

    scale = hd ** -0.5
    rix = lax.broadcasted_iota(jnp.int32, (HP, seq * kvh), 0)
    cix = lax.broadcasted_iota(jnp.int32, (HP, seq * kvh), 1)
    own_kv = lax.rem(cix, kvh) == lax.div(rix, group)
    colpos = jnp.where(own_kv, lax.div(cix, kvh), 2 * seq)

    def blk(hf, i):
        return pl.ds(pl.multiple_of(hf * hrows + i * ht, ht), ht)

    def hblk(hf, i, s):
        return pl.ds(pl.multiple_of(hf * hrows + i * ht + s * half, half), half)

    hp_pieces = kpieces // HALVES

    def attention(l, hf, hooks):
        trow = slice(hf * ht, (hf + 1) * ht)

        def rotate(v):
            return v * cos_scr[trow, :] + pltpu.roll(v, half_hd, 1) * sin_scr[trow, :]

        def first(i):
            if hf == 0:
                w_copy(l, i).wait()

        xf32 = xs[trow, :]
        h = (xf32 * lax.rsqrt(jnp.mean(xf32 * xf32, axis=-1, keepdims=True) + EPSILON)).astype(BF16)
        first(0)
        per = 256 // hd
        for n in range(heads // per):
            qn = jnp.dot(h, wqb[:, n * 256:(n + 1) * 256], preferred_element_type=F32)
            for s in range(per):
                r = rotate(qn[:, s * hd:(s + 1) * hd]).astype(BF16).astype(F32)
                q_scr[pl.ds(n * per + s, ht, stride=HP), :] = r
        first(1)
        kn = jnp.dot(h, wkb[...], preferred_element_type=F32)
        first(2)
        vn = jnp.dot(h, wvb[...], preferred_element_type=F32)
        for kv in range(kvh):
            r = rotate(kn[:, kv * hd:(kv + 1) * hd]).astype(BF16).astype(F32)
            v = vn[:, kv * hd:(kv + 1) * hd].astype(BF16).astype(F32)
            for g in range(group):
                kn_scr[pl.ds(kv * group + g, ht, stride=HP), :] = r
                vn_scr[pl.ds(kv * group + g, ht, stride=HP), :] = v
        if l == 0 and hf == 0:
            for i in range(kpieces):
                v_copy(l, i).start()
            w_copy(l, 3).start()

        def qk(i, carry):
            for t in range(ht):
                r16 = pl.ds(pl.multiple_of(t * HP, HP), HP)
                q = q_scr[r16, :].astype(BF16)
                sc = lax.dot_general(q, kbuf[hf * ht + t], (((1,), (1,)), ((), ())), preferred_element_type=F32)
                s_scr[r16, :] = jnp.where(colpos < len_ref[pool * tok + hf * ht + t], sc * scale, -jnp.inf)
            return carry

        for i in range(hp_pieces):
            k_copy(l, hf * hp_pieces + i).wait()
        qk(0, 0)
        hooks[0]()
        if l == 0 and hf == 0:
            for t in range(R13):
                for cp in g_copies(t):
                    cp.start()

        def soft(i, carry):
            rr = pl.ds(pl.multiple_of(i * 128, 128), 128)
            sc = s_scr[rr, :]
            s_new = jnp.sum(q_scr[rr, :] * kn_scr[rr, :], axis=-1, keepdims=True) * scale
            peak = jnp.maximum(jnp.max(sc, axis=-1, keepdims=True), s_new)
            wts = jnp.exp(sc - peak)
            w_new = jnp.exp(s_new - peak)
            den = jnp.sum(wts, axis=-1, keepdims=True) + w_new
            p_scr[rr, :] = wts.astype(BF16)
            mn_scr[rr, :] = w_new.astype(BF16).astype(F32) * vn_scr[rr, :]
            den_scr[rr, :] = jnp.broadcast_to(den, (128, hd))
            return carry

        lax.fori_loop(0, ht * HP // 128, soft, 0)
        hooks[1]()

        def pv(i, carry):
            for t in range(ht):
                r16 = pl.ds(pl.multiple_of(t * HP, HP), HP)
                m = jnp.dot(p_scr[r16, :], vbuf[hf * ht + t], preferred_element_type=F32)
                mn_scr[r16, :] = ((m + mn_scr[r16, :]) / den_scr[r16, :]).astype(BF16).astype(F32)
            return carry

        for i in range(hp_pieces):
            v_copy(l, hf * hp_pieces + i).wait()
        pv(0, 0)
        att = jnp.concatenate([mn_scr[pl.ds(h, ht, stride=HP), :].astype(BF16) for h in range(heads)], axis=1)
        first(3)
        for n in range(model // 256):
            cs = slice(n * 256, (n + 1) * 256)
            a_scr[trow, cs] = (xs[trow, cs] + jnp.dot(att, wob[:, cs], preferred_element_type=F32)).astype(BF16).astype(F32)
        a = a_scr[trow, :]
        u = (a * lax.rsqrt(jnp.mean(a * a, axis=-1, keepdims=True) + EPSILON)).astype(BF16)
        u_all[blk(hf, e), :] = u
        parts = lax.dot_general(wr3[l], u, (((1,), (1,)), ((), ())), preferred_element_type=F32)
        logits = (parts[2 * nexp:3 * nexp] + parts[nexp:2 * nexp]) + parts[0:nexp]
        ids = ids_ref[l]
        mine = ids[:, hf * ht:(hf + 1) * ht]
        for i in range(1, npool):
            mine = jnp.where(pool == i, ids[:, i * tok + hf * ht:i * tok + (hf + 1) * ht], mine)
        eix = lax.broadcasted_iota(jnp.int32, (nexp, ht), 0)
        hit = eix == mine[0:1, :]
        for k in range(1, topk):
            hit = jnp.logical_or(hit, eix == mine[k:k + 1, :])
        ml = jnp.where(hit, logits, -jnp.inf)
        ex = jnp.exp(ml - jnp.max(ml, axis=0, keepdims=True))
        gates = ex / jnp.sum(ex, axis=0, keepdims=True)
        g_all[hf, e] = jnp.concatenate([gates, jnp.zeros((nexp, LANES - ht), F32)], axis=1)

    def dcopies(hf, i):
        dev = to_ep((partner, er, el, er, el, partner, partner, dr, dl)[i])
        rws = (blk(hf, e), blk(hf, e), blk(hf, e), hblk(hf, el, 0), hblk(hf, er, 1), blk(hf, el), blk(hf, er),
               hblk(hf, el, 0), hblk(hf, er, 1))[i]
        gix = (e, e, e, el, None, el, er, el, None)[i]
        a = pltpu.make_async_remote_copy(src_ref=u_all.at[rws], dst_ref=u_all.at[rws], send_sem=du_s.at[hf, i],
                                         recv_sem=du_r.at[hf, i], device_id=dev, device_id_type=MESH)
        if gix is None:
            return (a,)
        b = pltpu.make_async_remote_copy(src_ref=g_all.at[hf, gix], dst_ref=g_all.at[hf, gix], send_sem=dg_s.at[hf, i],
                                         recv_sem=dg_r.at[hf, i], device_id=dev, device_id_type=MESH)
        return (a, b)

    def start(cs):
        for cp in cs:
            cp.start()

    def wait_recv(cs):
        for cp in cs:
            cp.wait_recv()

    def wait_send(cs):
        for cp in cs:
            cp.wait_send()

    def disp1(hf):
        for i in (1, 2, 0):
            start(dcopies(hf, i))

    def disp2(hf):
        for i, js in ((1, (3, 7, 5)), (2, (4, 8, 6))):
            wait_recv(dcopies(hf, i))
            for j in js:
                start(dcopies(hf, j))

    def disp3(hf):
        for i in (0, 3, 4, 5, 6, 7, 8):
            wait_recv(dcopies(hf, i))
        for i in range(9):
            wait_send(dcopies(hf, i))
        gt = jnp.transpose(g_all[hf].reshape(ep * nexp, LANES))
        gt = gt[0:ht, :]
        lix = lax.broadcasted_iota(jnp.int32, (ht, ep * nexp), 1)
        for i in range(nloc):
            for b in range(ep):
                col = jnp.sum(jnp.where(lix == b * nexp + e * nloc + i, gt, 0.0), axis=1, keepdims=True)
                gcol[i, pl.ds(hf * hrows + b * ht, ht), :] = jnp.broadcast_to(col, (ht, LANES))

    def experts(l, i, hf, hooks):
        base13 = (l * npass + i * HALVES + hf) * n13
        t2 = l * nloc + i
        rws = slice(hf * hrows, (hf + 1) * hrows)

        def up(j, carry):
            t = base13 + j
            slot = lax.rem(t, R13)
            for cp in g_copies(t):
                cp.wait()
            hh = jnp.dot(u_all[rws, :], w13[slot], preferred_element_type=F32)
            gate = hh[:, 0:NW]
            act = gate * jax.nn.sigmoid(gate) * hh[:, NW:2 * NW]
            inner[:, pl.ds(pl.multiple_of(j * NW, NW), NW)] = act.astype(BF16)

            @pl.when(t + R13 < tot13)
            def _():
                for cp in g_copies(t + R13):
                    cp.start()
            for at, fn in hooks:
                pl.when(j == at)(fn)
            return carry

        lax.fori_loop(0, n13, up, 0)

        if hf == 0:
            d_copy(t2).wait()
        y = jnp.dot(inner[...], w2b[...], preferred_element_type=F32).astype(BF16).astype(F32)
        gc = gcol[i, rws, :]
        for s in range(model // LANES):
            cols = slice(s * LANES, (s + 1) * LANES)
            term = jnp.where(gc > 0.0, gc * y[:, cols], 0.0)
            if i == 0:
                psum[rws, cols] = term
            else:
                psum[rws, cols] = psum[rws, cols] + term
        if hf == HALVES - 1 and t2 + 1 < tot2:
            d_copy(t2 + 1).start()

    order = (xf, xr, xl, xx)

    def pcopy(hf, k):
        return pltpu.make_async_remote_copy(src_ref=psum.at[blk(hf, order[k] * CORES + oc)], dst_ref=pairbuf.at[hf, k],
                                            send_sem=pr_s.at[hf, k], recv_sem=pr_r.at[hf, k], device_id=to_ep(partner),
                                            device_id_type=MESH)

    def rcopy(hf, i):
        rws = (hblk(hf, ef, 1), hblk(hf, ef, 0), hblk(hf, er, 0), hblk(hf, el, 1), hblk(hf, er, 1), hblk(hf, el, 0))[i]
        return pltpu.make_async_remote_copy(src_ref=psum.at[rws], dst_ref=rbuf.at[hf, i], send_sem=rr_s.at[hf, i],
                                            recv_sem=rr_r.at[hf, i], device_id=to_ep(er if i % 2 == 0 else el), device_id_type=MESH)

    def ret1(hf):
        for k in range(nx):
            pcopy(hf, k).start()

    def ret2(hf, ks):
        for k in ks:
            pcopy(hf, k).wait_recv()
            rws = blk(hf, order[k] * CORES + c)
            psum[rws, :] = psum[rws, :] + pairbuf[hf, k]
            for m in ((0, 1), (2,), (3,), ())[k]:
                rcopy(hf, m).start()

    def ret3(hf):
        for m, rws, nxt in ((0, hblk(hf, er, 1), 4), (1, hblk(hf, el, 0), 5)):
            rcopy(hf, m).wait_recv()
            psum[rws, :] = psum[rws, :] + rbuf[hf, m]
            rcopy(hf, nxt).start()

    def ret4(hf):
        for s, m, n in ((0, 2, 5), (1, 3, 4)):
            rcopy(hf, m).wait_recv()
            rcopy(hf, n).wait_recv()
            part = psum[hblk(hf, e, s), :] + rbuf[hf, m] + rbuf[hf, n]
            tr = slice(hf * ht + s * half, hf * ht + (s + 1) * half)
            xs[tr, :] = (a_scr[tr, :] + part).astype(BF16).astype(F32)
        for k in range(nx):
            pcopy(hf, k).wait_send()
        for m in range(6):
            rcopy(hf, m).wait_send()

    def fblk(hf, i):
        return pl.ds(pl.multiple_of(i * tok + hf * ht, ht), ht)

    def fhblk(hf, i, s):
        return pl.ds(pl.multiple_of(i * tok + hf * ht + s * half, half), half)

    def fcopy(hf, i):
        rws = (fblk(hf, pool), fblk(hf, pool), fhblk(hf, pp, 0), fhblk(hf, pn, 1))[i]
        return pltpu.make_async_remote_copy(src_ref=fin.at[rws], dst_ref=fin.at[rws], send_sem=fs.at[hf, i], recv_sem=fr.at[hf, i],
                                            device_id=to_pool(pn if i % 2 == 0 else pp), device_id_type=MESH)

    def ocopy(hf, k):
        i = (pool, pp, pn, pf)[k]
        return pltpu.make_async_copy(fin.at[fblk(hf, i)], out_hbm.at[fblk(hf, i)], sem_o.at[hf, k])

    def fin1(hf):
        fin[fblk(hf, pool), :] = xs[hf * ht:(hf + 1) * ht, :].astype(BF16)
        fcopy(hf, 0).start()
        fcopy(hf, 1).start()
        ocopy(hf, 0).start()

    def fin2(hf):
        for i in range(2):
            fcopy(hf, i).wait_recv()
            fcopy(hf, i + 2).start()
            ocopy(hf, i + 1).start()

    def fin3(hf):
        fcopy(hf, 2).wait_recv()
        fcopy(hf, 3).wait_recv()
        ocopy(hf, 3).start()
        for k in range(4):
            ocopy(hf, k).wait()
            fcopy(hf, k).wait_send()

    def nothing():
        pass

    for l in range(layers):
        attention(l, 0, (nothing if l == 0 else lambda: ret3(1), nothing))
        disp1(0)
        if l > 0:
            ret4(1)
        attention(l, 1, (lambda: disp2(0), nothing))
        disp1(1)
        if l == 0:
            d_copy(0).start()
        disp3(0)
        experts(l, 0, 0, ((n13 - 3, lambda: disp2(1)),))
        if l + 1 < layers:
            for k in range(4):
                w_copy(l + 1, k).start()
            for k in range(kpieces):
                k_copy(l + 1, k).start()
                v_copy(l + 1, k).start()
        disp3(1)
        experts(l, 0, 1, ())
        experts(l, 1, 0, ())
        ret1(0)
        experts(l, 1, 1, ((1, lambda: ret2(0, (0,))), (2, lambda: ret2(0, (1, 2, 3))), (n13 - 1, lambda: ret3(0))))
        ret1(1)
        ret2(1, (0,))
        ret4(0)
        if l + 1 == layers:
            fin1(0)
        ret2(1, (1, 2, 3))
    ret3(1)
    fin2(0)
    ret4(1)
    fin1(1)
    fin3(0)
    fin2(1)
    fin3(1)


def solution(mesh):
    npool = mesh.shape["pool"]
    ep = mesh.shape["ep"]
    nx = ep // CORES

    def body(hidden, k_cache, v_cache, lengths, expert_ids, w_query, w_key, w_value, w_out, w_router, w_gate, w_up, w_down):
        layers, local, seq, kvh, hd = k_cache.shape
        model = hidden.shape[1]
        tok = local // npool
        heads = w_query.shape[2] // hd
        nloc, _, ff = w_gate.shape[1:]
        nexp = w_router.shape[2]
        topk = expert_ids.shape[2]
        kc = k_cache.reshape(layers, local, seq * kvh, hd)
        vc = v_cache.reshape(layers, local, seq * kvh, hd)
        ids_t = expert_ids.transpose(0, 2, 1)
        wr_t = w_router.transpose(0, 2, 1)
        cfg = (layers, tok, model, heads, kvh, hd, seq, ff, nloc, nx, npool, nexp, topk)
        rows = ep * tok
        ht = tok // HALVES
        hbm = pl.BlockSpec(memory_space=pl.ANY)
        vmem = pl.BlockSpec(memory_space=pltpu.VMEM)
        smem = pl.BlockSpec(memory_space=pltpu.SMEM)
        kpieces = 8
        dma = pltpu.SemaphoreType.DMA
        scratch = [
            pltpu.VMEM((tok, model), BF16), pltpu.VMEM((tok, model), F32), pltpu.VMEM((tok, model), F32),
            pltpu.VMEM((ht * HP, hd), F32), pltpu.VMEM((ht * HP, hd), F32), pltpu.VMEM((ht * HP, hd), F32),
            pltpu.VMEM((ht * HP, hd), F32), pltpu.VMEM((ht * HP, hd), F32),
            pltpu.VMEM((ht * HP, seq * kvh), F32), pltpu.VMEM((ht * HP, seq * kvh), BF16),
            pltpu.VMEM((tok, hd), F32), pltpu.VMEM((tok, hd), F32), pltpu.VMEM((layers, 3 * nexp, model), BF16),
            pltpu.VMEM((tok, seq * kvh, hd), BF16), pltpu.VMEM((tok, seq * kvh, hd), BF16),
            pltpu.VMEM((model, heads * hd), BF16), pltpu.VMEM((model, kvh * hd), BF16), pltpu.VMEM((model, kvh * hd), BF16),
            pltpu.VMEM((heads * hd, model), BF16),
            pltpu.VMEM((R13, model, 2 * NW), BF16), pltpu.VMEM((ff, model), BF16),
            pltpu.VMEM((rows, model), BF16), pltpu.VMEM((HALVES, ep, nexp, LANES), F32), pltpu.VMEM((nloc, rows, LANES), F32),
            pltpu.VMEM((rows // HALVES, ff), BF16), pltpu.VMEM((rows, model), F32), pltpu.VMEM((HALVES, nx, ht, model), F32),
            pltpu.VMEM((HALVES, 6, ht // 2, model), F32), pltpu.VMEM((local, model), BF16),
            dma((1,)), dma((4,)), dma((kpieces,)), dma((kpieces,)), dma((R13,)), dma((R13,)), dma((1,)),
            dma((HALVES, 9)), dma((HALVES, 9)), dma((HALVES, 9)), dma((HALVES, 9)), dma((HALVES, nx)), dma((HALVES, nx)),
            dma((HALVES, 6)), dma((HALVES, 6)), dma((HALVES, 4)), dma((HALVES, 4)), dma((HALVES, npool)),
        ]
        call = pl.pallas_call(
            functools.partial(step_kernel, cfg),
            out_shape=jax.ShapeDtypeStruct((local, model), BF16),
            in_specs=[hbm, hbm, hbm, smem, vmem, hbm, hbm, hbm, hbm, vmem, hbm, hbm, hbm],
            out_specs=hbm,
            scratch_shapes=scratch,
            compiler_params=pltpu.CompilerParams(collective_id=0, has_side_effects=True, vmem_limit_bytes=66_000_000),
        )
        return call(hidden, kc, vc, lengths, ids_t, w_query, w_key, w_value, w_out, wr_t, w_gate, w_up, w_down)

    rows_spec = ("dp", "ep")
    in_specs = (P(rows_spec, None), P(None, rows_spec), P(None, rows_spec), P(rows_spec), P(None, rows_spec, None), P(), P(), P(), P(), P(), P(None, "ep"), P(None, "ep"), P(None, "ep"))
    return jax.shard_map(body, mesh=mesh, in_specs=in_specs, out_specs=P(rows_spec, None), check_vma=False)
```

```python
import functools

import jax
import jax.numpy as jnp
from jax import lax
from jax.experimental import pallas as pl
from jax.experimental.pallas import tpu as pltpu
from jax.sharding import PartitionSpec as P

EPSILON = 1e-6
ROPE_BASE = 10000.0
MESH = pl.DeviceIdType.MESH
F32 = jnp.float32
BF16 = jnp.bfloat16
CORES = 2
HP = 16
LANES = 128
NW = 896
HALVES = 2


def step_kernel(cfg, x_hbm, kc_hbm, vc_hbm, len_ref, ids_ref, wq_hbm, wk_hbm, wv_hbm, wo_hbm, wr_ref, wg_hbm, wu_hbm, wd_hbm,
                out_hbm,
                xin, xs, a_scr, q_scr, kn_scr, vn_scr, mn_scr, den_scr, s_scr, p_scr, cos_scr, sin_scr, wr3,
                kbuf, vbuf, wqb, wkb, wvb, wob, w13, w2b,
                u_all, g_all, gcol, inner, psum, pairbuf, rbuf, fin,
                sem_x, sem_w, sem_k, sem_v, sem_g, sem_u, sem_d,
                du_s, du_r, dg_s, dg_r, pr_s, pr_r, rr_s, rr_r, fs, fr, sem_o):
    layers, tok, model, heads, kvh, hd, seq, ff, nloc, nx, npool, nexp, topk = cfg
    ep = nx * CORES
    rows = ep * tok
    ht = tok // HALVES
    hrows = rows // HALVES
    half = ht // 2
    group = heads // kvh
    pool = lax.axis_index("pool")
    e = lax.axis_index("ep")
    xx = lax.div(e, CORES)
    c = lax.rem(e, CORES)
    oc = 1 - c
    xr = lax.rem(xx + 1, nx)
    xl = lax.rem(xx + nx - 1, nx)
    xf = lax.rem(xx + 2, nx)
    partner = xx * CORES + oc
    dr = xr * CORES + oc
    dl = xl * CORES + oc
    er = xr * CORES + c
    el = xl * CORES + c
    ef = xf * CORES + c
    pn = lax.rem(pool + 1, npool)
    pp = lax.rem(pool + npool - 1, npool)
    pf = lax.rem(pool + 2, npool)

    def to_ep(i):
        return {"ep": i}

    def to_pool(i):
        return {"pool": i}

    barrier = pltpu.get_barrier_semaphore()
    for dev in (to_ep(partner), to_ep(er), to_ep(el), to_ep(dr), to_ep(dl), to_pool(pn), to_pool(pp)):
        pl.semaphore_signal(barrier, inc=1, device_id=dev, device_id_type=MESH)

    kpieces = sem_k.shape[0]
    kp = tok // kpieces
    tok0 = pl.multiple_of(pool * tok, tok)

    def k_copy(l, i):
        return pltpu.make_async_copy(kc_hbm.at[l, pl.ds(tok0 + i * kp, kp)], kbuf.at[pl.ds(i * kp, kp)], sem_k.at[i])

    def v_copy(l, i):
        return pltpu.make_async_copy(vc_hbm.at[l, pl.ds(tok0 + i * kp, kp)], vbuf.at[pl.ds(i * kp, kp)], sem_v.at[i])

    def w_copy(l, i):
        src = (wq_hbm, wk_hbm, wv_hbm, wo_hbm)[i]
        dst = (wqb, wkb, wvb, wob)[i]
        return pltpu.make_async_copy(src.at[l], dst, sem_w.at[i])

    n13 = ff // NW
    npass = nloc * HALVES
    tot13 = layers * nloc * n13
    tot2 = layers * nloc

    def g_copies(t):
        li = lax.div(t, n13)
        slot = lax.rem(t, n13)
        l = lax.div(li, nloc)
        i = lax.rem(li, nloc)
        cols = pl.ds(pl.multiple_of(slot * NW, NW), NW)
        return (pltpu.make_async_copy(wg_hbm.at[l, i, :, cols], w13.at[slot, :, pl.ds(0, NW)], sem_g.at[slot]),
                pltpu.make_async_copy(wu_hbm.at[l, i, :, cols], w13.at[slot, :, pl.ds(NW, NW)], sem_u.at[slot]))

    def d_copy(t):
        return pltpu.make_async_copy(wd_hbm.at[lax.div(t, nloc), lax.rem(t, nloc)], w2b, sem_d.at[0])

    x_copy = pltpu.make_async_copy(x_hbm.at[pl.ds(tok0, tok)], xin, sem_x.at[0])
    x_copy.start()
    for i in range(3):
        w_copy(0, i).start()
    for i in range(kpieces):
        k_copy(0, i).start()

    lane = lax.broadcasted_iota(jnp.int32, (tok, hd), 1)
    pos_i = jnp.zeros((tok, hd), jnp.int32)
    row_i = lax.broadcasted_iota(jnp.int32, (tok, hd), 0)
    for t in range(tok):
        pos_i = jnp.where(row_i == t, len_ref[pool * tok + t], pos_i)
    half_hd = hd // 2
    pair = jnp.where(lane < half_hd, lane, lane - half_hd).astype(F32)
    freqs = jnp.exp(pair * (-2.0 / hd) * jnp.log(jnp.full((tok, hd), ROPE_BASE, F32)))
    angle = pos_i.astype(F32) * freqs
    cos_scr[...] = jnp.cos(angle)
    sn = jnp.sin(angle)
    sin_scr[...] = jnp.where(lane < half_hd, -sn, sn)
    for l in range(layers):
        w = wr_ref[l]
        hi = w.astype(BF16)
        r1 = w - hi.astype(F32)
        mid = r1.astype(BF16)
        lo = (r1 - mid.astype(F32)).astype(BF16)
        wr3[l, pl.ds(0, nexp), :] = hi
        wr3[l, pl.ds(nexp, nexp), :] = mid
        wr3[l, pl.ds(2 * nexp, nexp), :] = lo
    zero_rows = jnp.zeros((ht, hd), F32)
    for h in range(heads, HP):
        q_scr[pl.ds(h, ht, stride=HP), :] = zero_rows
        kn_scr[pl.ds(h, ht, stride=HP), :] = zero_rows
        vn_scr[pl.ds(h, ht, stride=HP), :] = zero_rows

    pl.semaphore_wait(barrier, 7)
    x_copy.wait()
    xs[...] = xin[...].astype(F32)

    scale = hd ** -0.5
    rix = lax.broadcasted_iota(jnp.int32, (HP, seq * kvh), 0)
    cix = lax.broadcasted_iota(jnp.int32, (HP, seq * kvh), 1)
    own_kv = lax.rem(cix, kvh) == lax.div(rix, group)
    colpos = jnp.where(own_kv, lax.div(cix, kvh), 2 * seq)

    def blk(hf, i):
        return pl.ds(pl.multiple_of(hf * hrows + i * ht, ht), ht)

    def hblk(hf, i, s):
        return pl.ds(pl.multiple_of(hf * hrows + i * ht + s * half, half), half)

    hp_pieces = kpieces // HALVES

    def attention(l, hf, hooks):
        trow = slice(hf * ht, (hf + 1) * ht)

        def rotate(v):
            return v * cos_scr[trow, :] + pltpu.roll(v, half_hd, 1) * sin_scr[trow, :]

        def first(i):
            if hf == 0:
                w_copy(l, i).wait()

        xf32 = xs[trow, :]
        h = (xf32 * lax.rsqrt(jnp.mean(xf32 * xf32, axis=-1, keepdims=True) + EPSILON)).astype(BF16)
        first(0)
        per = 256 // hd
        for n in range(heads // per):
            qn = jnp.dot(h, wqb[:, n * 256:(n + 1) * 256], preferred_element_type=F32)
            for s in range(per):
                r = rotate(qn[:, s * hd:(s + 1) * hd]).astype(BF16).astype(F32)
                q_scr[pl.ds(n * per + s, ht, stride=HP), :] = r
        first(1)
        kn = jnp.dot(h, wkb[...], preferred_element_type=F32)
        first(2)
        vn = jnp.dot(h, wvb[...], preferred_element_type=F32)
        for kv in range(kvh):
            r = rotate(kn[:, kv * hd:(kv + 1) * hd]).astype(BF16).astype(F32)
            v = vn[:, kv * hd:(kv + 1) * hd].astype(BF16).astype(F32)
            for g in range(group):
                kn_scr[pl.ds(kv * group + g, ht, stride=HP), :] = r
                vn_scr[pl.ds(kv * group + g, ht, stride=HP), :] = v
        if hf == 0:
            @pl.when(l == 0)
            def _():
                for i in range(kpieces):
                    v_copy(l, i).start()
                w_copy(l, 3).start()

        def qk(i, carry):
            for t in range(ht):
                r16 = pl.ds(pl.multiple_of(t * HP, HP), HP)
                q = q_scr[r16, :].astype(BF16)
                sc = lax.dot_general(q, kbuf[hf * ht + t], (((1,), (1,)), ((), ())), preferred_element_type=F32)
                s_scr[r16, :] = jnp.where(colpos < len_ref[pool * tok + hf * ht + t], sc * scale, -jnp.inf)
            return carry

        for i in range(hp_pieces):
            k_copy(l, hf * hp_pieces + i).wait()
        qk(0, 0)
        hooks[0]()
        if hf == 0:
            @pl.when(l == 0)
            def _():
                for t in range(n13):
                    for cp in g_copies(t):
                        cp.start()

        def soft(i, carry):
            rr = pl.ds(pl.multiple_of(i * 128, 128), 128)
            sc = s_scr[rr, :]
            s_new = jnp.sum(q_scr[rr, :] * kn_scr[rr, :], axis=-1, keepdims=True) * scale
            peak = jnp.maximum(jnp.max(sc, axis=-1, keepdims=True), s_new)
            wts = jnp.exp(sc - peak)
            w_new = jnp.exp(s_new - peak)
            den = jnp.sum(wts, axis=-1, keepdims=True) + w_new
            p_scr[rr, :] = wts.astype(BF16)
            mn_scr[rr, :] = w_new.astype(BF16).astype(F32) * vn_scr[rr, :]
            den_scr[rr, :] = jnp.broadcast_to(den, (128, hd))
            return carry

        lax.fori_loop(0, ht * HP // 128, soft, 0)
        hooks[1]()

        def pv(i, carry):
            for t in range(ht):
                r16 = pl.ds(pl.multiple_of(t * HP, HP), HP)
                m = jnp.dot(p_scr[r16, :], vbuf[hf * ht + t], preferred_element_type=F32)
                mn_scr[r16, :] = ((m + mn_scr[r16, :]) / den_scr[r16, :]).astype(BF16).astype(F32)
            return carry

        for i in range(hp_pieces):
            v_copy(l, hf * hp_pieces + i).wait()
        pv(0, 0)
        att = jnp.concatenate([mn_scr[pl.ds(h, ht, stride=HP), :].astype(BF16) for h in range(heads)], axis=1)
        first(3)
        for n in range(model // 256):
            cs = slice(n * 256, (n + 1) * 256)
            a_scr[trow, cs] = (xs[trow, cs] + jnp.dot(att, wob[:, cs], preferred_element_type=F32)).astype(BF16).astype(F32)
        a = a_scr[trow, :]
        u = (a * lax.rsqrt(jnp.mean(a * a, axis=-1, keepdims=True) + EPSILON)).astype(BF16)
        u_all[blk(hf, e), :] = u
        parts = lax.dot_general(wr3[l], u, (((1,), (1,)), ((), ())), preferred_element_type=F32)
        logits = (parts[2 * nexp:3 * nexp] + parts[nexp:2 * nexp]) + parts[0:nexp]
        ids = ids_ref[l]
        mine = ids[:, hf * ht:(hf + 1) * ht]
        for i in range(1, npool):
            mine = jnp.where(pool == i, ids[:, i * tok + hf * ht:i * tok + (hf + 1) * ht], mine)
        eix = lax.broadcasted_iota(jnp.int32, (nexp, ht), 0)
        hit = eix == mine[0:1, :]
        for k in range(1, topk):
            hit = jnp.logical_or(hit, eix == mine[k:k + 1, :])
        ml = jnp.where(hit, logits, -jnp.inf)
        ex = jnp.exp(ml - jnp.max(ml, axis=0, keepdims=True))
        gates = ex / jnp.sum(ex, axis=0, keepdims=True)
        g_all[hf, e] = jnp.concatenate([gates, jnp.zeros((nexp, LANES - ht), F32)], axis=1)

    def dcopies(hf, i):
        dev = to_ep((partner, er, el, er, el, partner, partner, dr, dl, er, el)[i])
        rws = (blk(hf, e), hblk(hf, e, 0), hblk(hf, e, 1), hblk(hf, el, 0), hblk(hf, er, 1), blk(hf, el), blk(hf, er),
               hblk(hf, el, 0), hblk(hf, er, 1), hblk(hf, e, 1), hblk(hf, e, 0))[i]
        gix = (e, e, e, el, None, el, er, el, None, None, None)[i]
        a = pltpu.make_async_remote_copy(src_ref=u_all.at[rws], dst_ref=u_all.at[rws], send_sem=du_s.at[hf, i],
                                         recv_sem=du_r.at[hf, i], device_id=dev, device_id_type=MESH)
        if gix is None:
            return (a,)
        b = pltpu.make_async_remote_copy(src_ref=g_all.at[hf, gix], dst_ref=g_all.at[hf, gix], send_sem=dg_s.at[hf, i],
                                         recv_sem=dg_r.at[hf, i], device_id=dev, device_id_type=MESH)
        return (a, b)

    def start(cs):
        for cp in cs:
            cp.start()

    def wait_recv(cs):
        for cp in cs:
            cp.wait_recv()

    def wait_send(cs):
        for cp in cs:
            cp.wait_send()

    def disp1(hf):
        for i in (1, 2, 9, 10, 0):
            start(dcopies(hf, i))

    def disp2(hf):
        for i, js in ((1, (3, 7)), (2, (4, 8))):
            wait_recv(dcopies(hf, i))
            for j in js:
                start(dcopies(hf, j))

    def disp3(hf):
        for i, j in ((9, 5), (10, 6)):
            wait_recv(dcopies(hf, i))
            start(dcopies(hf, j))

    def disp4(hf):
        for i in (0, 3, 4, 5, 6, 7, 8):
            wait_recv(dcopies(hf, i))
        for i in range(11):
            wait_send(dcopies(hf, i))
        gt = jnp.transpose(g_all[hf].reshape(ep * nexp, LANES))
        gt = gt[0:ht, :]
        lix = lax.broadcasted_iota(jnp.int32, (ht, ep * nexp), 1)
        for i in range(nloc):
            for b in range(ep):
                col = jnp.sum(jnp.where(lix == b * nexp + e * nloc + i, gt, 0.0), axis=1, keepdims=True)
                gcol[i, pl.ds(hf * hrows + b * ht, ht), :] = jnp.broadcast_to(col, (ht, LANES))

    def experts(l, q, hooks):
        i = lax.div(q, HALVES)
        hf = lax.rem(q, HALVES)
        t2 = l * nloc + i
        base13 = t2 * n13
        rws = pl.ds(pl.multiple_of(hf * hrows, hrows), hrows)

        def up(j, carry):
            t = base13 + j

            @pl.when(hf == 0)
            def _():
                for cp in g_copies(t):
                    cp.wait()

            hh = jnp.dot(u_all[rws, :], w13[j], preferred_element_type=F32)
            gate = hh[:, 0:NW]
            act = gate * jax.nn.sigmoid(gate) * hh[:, NW:2 * NW]
            inner[:, pl.ds(pl.multiple_of(j * NW, NW), NW)] = act.astype(BF16)

            @pl.when(jnp.logical_and(hf == HALVES - 1, t + n13 < tot13))
            def _():
                for cp in g_copies(t + n13):
                    cp.start()
            for qa, at, fn in hooks:
                pl.when(jnp.logical_and(q == qa, j == at))(fn)
            return carry

        lax.fori_loop(0, n13, up, 0)

        @pl.when(hf == 0)
        def _():
            d_copy(t2).wait()

        y = jnp.dot(inner[...], w2b[...], preferred_element_type=F32).astype(BF16).astype(F32)
        gc = gcol[i, rws, :]
        for s in range(model // LANES):
            cols = slice(s * LANES, (s + 1) * LANES)
            term = jnp.where(gc > 0.0, gc * y[:, cols], 0.0)
            psum[rws, cols] = jnp.where(i == 0, 0.0, psum[rws, cols]) + term

        @pl.when(jnp.logical_and(hf == HALVES - 1, t2 + 1 < tot2))
        def _():
            d_copy(t2 + 1).start()

    order = (xf, xr, xl, xx)

    def pcopy(hf, k):
        return pltpu.make_async_remote_copy(src_ref=psum.at[blk(hf, order[k] * CORES + oc)], dst_ref=pairbuf.at[hf, k],
                                            send_sem=pr_s.at[hf, k], recv_sem=pr_r.at[hf, k], device_id=to_ep(partner),
                                            device_id_type=MESH)

    def rcopy(hf, i):
        rws = (hblk(hf, ef, 1), hblk(hf, ef, 0), hblk(hf, er, 0), hblk(hf, el, 1), hblk(hf, er, 1), hblk(hf, el, 0))[i]
        return pltpu.make_async_remote_copy(src_ref=psum.at[rws], dst_ref=rbuf.at[hf, i], send_sem=rr_s.at[hf, i],
                                            recv_sem=rr_r.at[hf, i], device_id=to_ep(er if i % 2 == 0 else el), device_id_type=MESH)

    def ret1(hf):
        for k in range(nx):
            pcopy(hf, k).start()

    def ret2(hf, ks):
        for k in ks:
            pcopy(hf, k).wait_recv()
            rws = blk(hf, order[k] * CORES + c)
            psum[rws, :] = psum[rws, :] + pairbuf[hf, k]
            for m in ((0, 1), (2,), (3,), ())[k]:
                rcopy(hf, m).start()

    def ret3(hf):
        for m, rws, nxt in ((0, hblk(hf, er, 1), 4), (1, hblk(hf, el, 0), 5)):
            rcopy(hf, m).wait_recv()
            psum[rws, :] = psum[rws, :] + rbuf[hf, m]
            rcopy(hf, nxt).start()

    def ret4(hf):
        for s, m, n in ((0, 2, 5), (1, 3, 4)):
            rcopy(hf, m).wait_recv()
            rcopy(hf, n).wait_recv()
            part = psum[hblk(hf, e, s), :] + rbuf[hf, m] + rbuf[hf, n]
            tr = slice(hf * ht + s * half, hf * ht + (s + 1) * half)
            xs[tr, :] = (a_scr[tr, :] + part).astype(BF16).astype(F32)
        for k in range(nx):
            pcopy(hf, k).wait_send()
        for m in range(6):
            rcopy(hf, m).wait_send()

    def fblk(hf, i):
        return pl.ds(pl.multiple_of(i * tok + hf * ht, ht), ht)

    def fhblk(hf, i, s):
        return pl.ds(pl.multiple_of(i * tok + hf * ht + s * half, half), half)

    def fcopy(hf, i):
        rws = (fhblk(hf, pool, 0), fhblk(hf, pool, 1), fhblk(hf, pp, 0), fhblk(hf, pn, 1), fhblk(hf, pool, 1), fhblk(hf, pool, 0))[i]
        return pltpu.make_async_remote_copy(src_ref=fin.at[rws], dst_ref=fin.at[rws], send_sem=fs.at[hf, i], recv_sem=fr.at[hf, i],
                                            device_id=to_pool(pn if i % 2 == 0 else pp), device_id_type=MESH)

    def ocopy(hf, k):
        i = (pool, pp, pn, pf)[k]
        return pltpu.make_async_copy(fin.at[fblk(hf, i)], out_hbm.at[fblk(hf, i)], sem_o.at[hf, k])

    def fin1(hf):
        fin[fblk(hf, pool), :] = xs[hf * ht:(hf + 1) * ht, :].astype(BF16)
        for i in (0, 1, 4, 5):
            fcopy(hf, i).start()
        ocopy(hf, 0).start()

    def fin2(hf):
        for i in range(2):
            fcopy(hf, i).wait_recv()
            fcopy(hf, i + 2).start()
        for i in range(2):
            fcopy(hf, i + 4).wait_recv()
            ocopy(hf, i + 1).start()

    def fin3(hf):
        fcopy(hf, 2).wait_recv()
        fcopy(hf, 3).wait_recv()
        ocopy(hf, 3).start()
        for k in range(4):
            ocopy(hf, k).wait()
        for k in range(6):
            fcopy(hf, k).wait_send()

    def nothing():
        pass

    def layer(l, carry):
        later = l > 0
        last = l == layers - 1

        attention(l, 0, (lambda: pl.when(later)(lambda: ret3(1)), nothing))
        disp1(0)
        pl.when(later)(lambda: ret4(1))
        attention(l, 1, (lambda: disp2(0), lambda: disp3(0)))
        disp1(1)
        pl.when(l == 0)(lambda: d_copy(0).start())
        disp4(0)

        def next_loads():
            for k in range(4):
                w_copy(l + 1, k).start()
            for k in range(kpieces):
                k_copy(l + 1, k).start()
                v_copy(l + 1, k).start()

        end = npass - 1
        hooks = ((0, n13 - 2, lambda: disp2(1)), (0, n13 - 1, lambda: disp3(1)), (end, 0, lambda: ret2(0, (0,))),
                 (end, n13 - 2, lambda: ret2(0, (1, 2, 3))), (end, n13 - 1, lambda: ret3(0)))

        def one_pass(q, c2):
            pl.when(q == 1)(lambda: disp4(1))
            pl.when(q == end)(lambda: ret1(0))
            experts(l, q, hooks)
            pl.when(jnp.logical_and(q == 0, l + 1 < layers))(next_loads)
            return c2

        lax.fori_loop(0, npass, one_pass, 0)
        ret1(1)
        ret2(1, (0,))
        ret4(0)
        pl.when(last)(lambda: fin1(0))
        ret2(1, (1, 2, 3))
        return carry

    lax.fori_loop(0, layers, layer, 0)
    ret3(1)
    fin2(0)
    ret4(1)
    fin1(1)
    fin3(0)
    fin2(1)
    fin3(1)


def solution(mesh):
    npool = mesh.shape["pool"]
    ep = mesh.shape["ep"]
    nx = ep // CORES

    def body(hidden, k_cache, v_cache, lengths, expert_ids, w_query, w_key, w_value, w_out, w_router, w_gate, w_up, w_down):
        layers, local, seq, kvh, hd = k_cache.shape
        model = hidden.shape[1]
        tok = local // npool
        heads = w_query.shape[2] // hd
        nloc, _, ff = w_gate.shape[1:]
        nexp = w_router.shape[2]
        topk = expert_ids.shape[2]
        kc = k_cache.reshape(layers, local, seq * kvh, hd)
        vc = v_cache.reshape(layers, local, seq * kvh, hd)
        ids_t = expert_ids.transpose(0, 2, 1)
        wr_t = w_router.transpose(0, 2, 1)
        cfg = (layers, tok, model, heads, kvh, hd, seq, ff, nloc, nx, npool, nexp, topk)
        rows = ep * tok
        ht = tok // HALVES
        hbm = pl.BlockSpec(memory_space=pl.ANY)
        vmem = pl.BlockSpec(memory_space=pltpu.VMEM)
        smem = pl.BlockSpec(memory_space=pltpu.SMEM)
        kpieces = 8
        dma = pltpu.SemaphoreType.DMA
        scratch = [
            pltpu.VMEM((tok, model), BF16), pltpu.VMEM((tok, model), F32), pltpu.VMEM((tok, model), F32),
            pltpu.VMEM((ht * HP, hd), F32), pltpu.VMEM((ht * HP, hd), F32), pltpu.VMEM((ht * HP, hd), F32),
            pltpu.VMEM((ht * HP, hd), F32), pltpu.VMEM((ht * HP, hd), F32),
            pltpu.VMEM((ht * HP, seq * kvh), F32), pltpu.VMEM((ht * HP, seq * kvh), BF16),
            pltpu.VMEM((tok, hd), F32), pltpu.VMEM((tok, hd), F32), pltpu.VMEM((layers, 3 * nexp, model), BF16),
            pltpu.VMEM((tok, seq * kvh, hd), BF16), pltpu.VMEM((tok, seq * kvh, hd), BF16),
            pltpu.VMEM((model, heads * hd), BF16), pltpu.VMEM((model, kvh * hd), BF16), pltpu.VMEM((model, kvh * hd), BF16),
            pltpu.VMEM((heads * hd, model), BF16),
            pltpu.VMEM((ff // NW, model, 2 * NW), BF16), pltpu.VMEM((ff, model), BF16),
            pltpu.VMEM((rows, model), BF16), pltpu.VMEM((HALVES, ep, nexp, LANES), F32), pltpu.VMEM((nloc, rows, LANES), F32),
            pltpu.VMEM((rows // HALVES, ff), BF16), pltpu.VMEM((rows, model), F32), pltpu.VMEM((HALVES, nx, ht, model), F32),
            pltpu.VMEM((HALVES, 6, ht // 2, model), F32), pltpu.VMEM((local, model), BF16),
            dma((1,)), dma((4,)), dma((kpieces,)), dma((kpieces,)), dma((ff // NW,)), dma((ff // NW,)), dma((1,)),
            dma((HALVES, 11)), dma((HALVES, 11)), dma((HALVES, 11)), dma((HALVES, 11)), dma((HALVES, nx)), dma((HALVES, nx)),
            dma((HALVES, 6)), dma((HALVES, 6)), dma((HALVES, 6)), dma((HALVES, 6)), dma((HALVES, npool)),
        ]
        call = pl.pallas_call(
            functools.partial(step_kernel, cfg),
            out_shape=jax.ShapeDtypeStruct((local, model), BF16),
            in_specs=[hbm, hbm, hbm, smem, vmem, hbm, hbm, hbm, hbm, vmem, hbm, hbm, hbm],
            out_specs=hbm,
            scratch_shapes=scratch,
            compiler_params=pltpu.CompilerParams(collective_id=0, has_side_effects=True, vmem_limit_bytes=66_000_000),
        )
        return call(hidden, kc, vc, lengths, ids_t, w_query, w_key, w_value, w_out, wr_t, w_gate, w_up, w_down)

    rows_spec = ("dp", "ep")
    in_specs = (P(rows_spec, None), P(None, rows_spec), P(None, rows_spec), P(rows_spec), P(None, rows_spec, None), P(), P(), P(), P(), P(), P(None, "ep"), P(None, "ep"), P(None, "ep"))
    return jax.shard_map(body, mesh=mesh, in_specs=in_specs, out_specs=P(rows_spec, None), check_vma=False)
```
